32 devices in a mesh: gx: 4 (over z), gy: 8 (over y, x, core).
Axes of the slice: x: 2, y: 2, z: 4, core: 2. Of those that a mesh axis runs over, the one named last changes fastest.
Arguments:
- probes: float32 [8, 64, 128, 512], P(None, 'gx', 'gy'), may hold values from -12.5 to 12.5, as said below
- disorder: float32 [64, 128, 512], P('gx', 'gy'), may hold values from -2 to 2
- spectrum_center: float32 [1], replicated, may hold values from -0.5 to 0.5
- half_width: float32 [1], replicated, may hold values from 9 to 11
Outputs:
- last_vector: float32 [8, 64, 128, 512], P(None, 'gx', 'gy')
- moments: float32 [8, 8], replicated
The draws below stay inside these ranges and needn't reach their ends.
Inputs may be any that keep to these rules, and one draw needn't show every extreme that they name: `probes`: real-valued probe entries.
All inputs are finite; a program needn't handle non-finite values.
Results may differ from the reference program's by a relative error of at most 0.0001.
Values sent between devices are 32-bit elements; how exact they have to be, the bound alone decides.
A program may use at most 128 MiB of HBM per device.

```python
import jax
import jax.numpy as jnp

PROBES = 8
NZ = 512
STEPS = 4
NX = 64
NY = 128


def draw_probes(key, part):
    first, second = jax.random.split(key, 2)
    shape = (PROBES, NX, NY, NZ)
    rough = jnp.exp(jax.random.uniform(second, shape, jnp.float32, -0.7, 0.7))
    rows_x = jnp.arange(NX, dtype=jnp.float32)[:, None]
    rows_y = jnp.arange(NY, dtype=jnp.float32)[None, :]
    frac = (rows_x * NY + rows_y) / (NX * NY - 1.0)
    base = jnp.clip(jax.random.normal(first, shape, jnp.float32), -4.0, 4.0)
    ramp = 0.5 + frac
    return (base * rough * ramp[None, :, :, None]).astype(jnp.float32)


def block_scale(rng, dims, shards, smallest, high):
    loudness, own = 1.0, jax.random.fold_in(rng, 6)
    for dim, parts in shards:
        heights = jnp.exp(jax.random.uniform(jax.random.fold_in(own, dim), (parts,), jnp.float32, smallest / len(shards), high / len(shards)))
        loudness = loudness * jnp.repeat(heights, dims[dim] // parts).reshape([-1 if axis == dim else 1 for axis in range(len(dims))])
    return loudness


def setup_inputs(seed: int = 0) -> dict:
    key_of = jax.random.split(jax.random.key(seed), 5)
    return {
        "probes": draw_probes(jax.random.fold_in(key_of[4], 71), 0),
        "disorder": jnp.clip(jax.random.uniform(key_of[1], (NX, NY, NZ), jnp.float32, -2.0, 2.0) * block_scale(key_of[1], (NX, NY, NZ), ((0, 4), (1, 8)), -0.4, 0.0), -2.0, 2.0),
        "spectrum_center": jnp.clip(jax.random.uniform(key_of[2], (1,), jnp.float32, -0.5, 0.5), -0.5, 0.5),
        "half_width": jnp.clip(jax.random.uniform(key_of[3], (1,), jnp.float32, 9.0, 11.0), 9.0, 11.0),
    }


def scaled_apply(ext, eps_part, center, width):
    core = ext[:, 1:-1, 1:-1]
    beside = ext[:, 2:, 1:-1] + ext[:, :-2, 1:-1] + ext[:, 1:-1, 2:] + ext[:, 1:-1, :-2]
    beside = beside + jnp.roll(core, 1, 3) + jnp.roll(core, -1, 3)
    return ((eps_part - center) * core - beside) / width


def padded(field):
    return jnp.pad(field, ((0, 0), (1, 1), (1, 1), (0, 0)), mode="wrap")


def inner_pair(t_low, t_high):
    square = jnp.sum(t_low * t_low, axis=(1, 2, 3))
    cross = jnp.sum(t_high * t_low, axis=(1, 2, 3))
    return jnp.stack([square, cross])


def reference(probes, disorder, spectrum_center, half_width):
    center = spectrum_center[0]
    width = half_width[0]
    energy = disorder[None]
    t_low = probes
    t_high = scaled_apply(padded(t_low), energy, center, width)
    collected = []
    for step in range(STEPS):
        collected.append(inner_pair(t_low, t_high))
        if step + 1 < STEPS:
            t_next = 2.0 * scaled_apply(padded(t_high), energy, center, width) - t_low
            t_low, t_high = t_high, t_next
    stacked = jnp.stack(collected)
    sites = jnp.float32(NX * NY * NZ)
    square = stacked[:, 0, :] / sites
    cross = stacked[:, 1, :] / sites
    even = 2.0 * square - square[0]
    odd = 2.0 * cross - cross[0]
    moments = jnp.stack([even, odd], axis=1).reshape(2 * STEPS, -1).T
    return t_high, moments
```

```python
import functools

import jax
import jax.numpy as jnp
from jax import lax
from jax.experimental import pallas as pl
from jax.experimental.pallas import tpu as pltpu
from jax.sharding import PartitionSpec as P

STEPS = 4
MESH = pl.DeviceIdType.MESH
ROWS = 8
LEAD = 2
GATE = 4
SPLIT = 2


def kernel(counts, sites, probes_hbm, disorder_hbm, center, width, last, moments, *scratch):
    fields = scratch[:STEPS]
    (disorder, near, faces, coef, acc, gather_x, gather_y, load_sem, face_sem, energy_sem, up_sem, down_sem,
     xs_sem, ys_sem, xr_sem, yr_sem, hr_sem, gxs_sem, gxr_sem, gys_sem, gyr_sem) = scratch[STEPS:]
    n_probes, nx, ny, nz = probes_hbm.shape
    tiles = ny // ROWS
    count_x, count_y = counts
    me_x = lax.axis_index("gx")
    me_y = lax.axis_index("gy")

    top = count_x - 1

    def at_x(offset):
        return (lax.rem(me_x + offset, count_x), me_y)

    def at_y(offset):
        return (me_x, lax.rem(me_y + offset, count_y))

    def load_face(row):
        return pltpu.make_async_copy(
            probes_hbm.at[:, pl.ds(row, 1)], fields[0].at[:, pl.ds(row + 1, 1)], face_sem)

    def load(p):
        return pltpu.make_async_copy(
            probes_hbm.at[p, pl.ds(1, nx - 2)], fields[0].at[p, pl.ds(2, nx - 2)], load_sem)

    def arrived(ref, sem):
        pltpu.make_async_copy(ref, ref, sem).wait()

    def to_high(s, p):
        final_step = s + 1 == STEPS
        return pltpu.make_async_remote_copy(
            fields[s].at[p, 1], fields[s].at[p, nx + 1], xs_sem.at[s],
            hr_sem.at[p] if final_step else xr_sem.at[s % 2, p], device_id=at_x(count_x - 1), device_id_type=MESH)

    def to_low(s, p):
        return pltpu.make_async_remote_copy(
            fields[s].at[p, nx], fields[s].at[p, 0], xs_sem.at[s], xr_sem.at[s % 2, p],
            device_id=at_x(1), device_id_type=MESH)

    def y_sends(s, p):
        return (
            pltpu.make_async_remote_copy(
                faces.at[s, 0, p], near.at[s, 1, p], ys_sem.at[s], yr_sem.at[s % 2, p],
                device_id=at_y(count_y - 1), device_id_type=MESH),
            pltpu.make_async_remote_copy(
                faces.at[s, 1, p], near.at[s, 0, p], ys_sem.at[s], yr_sem.at[s % 2, p],
                device_id=at_y(1), device_id_type=MESH),
        )

    barrier = pltpu.get_barrier_semaphore()

    @pl.when(me_x < top)
    def _():
        pl.semaphore_signal(barrier, inc=1, device_id=(me_x + 1, me_y), device_id_type=MESH)

    @pl.when(me_x > 0)
    def _():
        pl.semaphore_signal(barrier, inc=1, device_id=(me_x - 1, me_y), device_id_type=MESH)

    for offset in range(1, count_y):
        pl.semaphore_signal(barrier, inc=1, device_id=at_y(offset), device_id_type=MESH)

    for row in (0, nx - 1):
        load_face(row).start()

    @pl.loop(0, n_probes)
    def _(p):
        load(p).start()

    energy = pltpu.make_async_copy(disorder_hbm, disorder, energy_sem)
    energy.start()

    arrived(fields[0].at[:, pl.ds(0, 2)], face_sem)
    pl.semaphore_wait(barrier, count_y - 1 + (me_x < top).astype(jnp.int32) + (me_x > 0).astype(jnp.int32))

    if count_x > 2:
        @pl.when(me_x == 1)
        def _():
            pl.semaphore_signal(up_sem, inc=1, device_id=(me_x + 1, me_y), device_id_type=MESH)

        @pl.when(me_x == top - 1)
        def _():
            pl.semaphore_signal(down_sem, inc=1, device_id=(me_x - 1, me_y), device_id_type=MESH)

    def adjacent_sends(p):
        @pl.when(me_x < top)
        def _():
            to_low(0, p).start()

        @pl.when(me_x > 0)
        def _():
            to_high(0, p).start()

    def wrapped_sends(p):
        @pl.when(me_x == top)
        def _():
            to_low(0, p).start()

        @pl.when(me_x == 0)
        def _():
            to_high(0, p).start()

    lead = min(LEAD, n_probes)
    pl.loop(0, lead)(adjacent_sends)

    if count_x > 2:
        @pl.when(me_x > 1)
        def _():
            pl.semaphore_wait(up_sem, 1)

            @pl.when(me_x < top)
            def _():
                pl.semaphore_signal(up_sem, inc=1, device_id=(me_x + 1, me_y), device_id_type=MESH)

        @pl.when(me_x < top - 1)
        def _():
            pl.semaphore_wait(down_sem, 1)

            @pl.when(me_x > 0)
            def _():
                pl.semaphore_signal(down_sem, inc=1, device_id=(me_x - 1, me_y), device_id_type=MESH)

    @pl.loop(lead, n_probes)
    def _(p):
        adjacent_sends(p)
        wrapped_sends(p - lead)

    pl.loop(n_probes - lead, n_probes)(wrapped_sends)
    arrived(fields[0].at[:, pl.ds(2, nx - 2)], load_sem)

    @pl.loop(0, n_probes)
    def _(p):
        @pl.loop(0, nx)
        def _(x):
            faces[0, 0, p, x] = fields[0][p, x + 1, pl.ds(0, 1)]
            faces[0, 1, p, x] = fields[0][p, x + 1, pl.ds(ny - 1, 1)]

        for copy in y_sends(0, p):
            copy.start()

    scale = 2.0 / jnp.full((ROWS, nz), width[0], jnp.float32)
    middle = center[0]
    energy.wait()

    @pl.loop(0, nx)
    def _(x):
        for i in range(tiles):
            part = pl.ds(ROWS * i, ROWS)
            coef[x, part] = (disorder[x, part] - middle) * scale

    sub = lax.broadcasted_iota(jnp.int32, (ROWS, nz), 0)
    first = sub == 0
    final = sub == ROWS - 1
    lanes = lax.broadcasted_iota(jnp.int32, (n_probes, 128), 1)
    sums = jnp.zeros((n_probes, 128), jnp.float32)

    def fold(v):
        parts = [v[:, 128 * j:128 * (j + 1)] for j in range(nz // 128)]
        while len(parts) > 1:
            parts = [a + b for a, b in zip(parts[::2], parts[1::2])] + (
                [parts[-1]] if len(parts) % 2 else [])
        return parts[0]

    for s in range(STEPS):
        cur = fields[s]
        final_step = s + 1 == STEPS

        @pl.loop(0, n_probes)
        def _(p):
            if final_step:
                to_low(s, p).wait_recv()

                @pl.when(p >= GATE)
                def _():
                    to_high(s, p - GATE).start()
            else:
                arrived(cur.at[p, pl.ds(0, 2)], xr_sem.at[s % 2, p])
            arrived(near.at[s, :, p], yr_sem.at[s % 2, p])

            def row(x, carry, edge=False):
                square, cross = carry
                low = jnp.broadcast_to(near[s, 0, p, x], (ROWS, nz))
                high = jnp.broadcast_to(near[s, 1, p, x], (ROWS, nz))
                here = [cur[p, x + 1, pl.ds(ROWS * i, ROWS)] for i in range(tiles)]
                down = [pltpu.roll(v, 1, 0) for v in here]
                up = [pltpu.roll(v, ROWS - 1, 0) for v in here]
                for i in range(tiles):
                    part = pl.ds(ROWS * i, ROWS)
                    v = here[i]
                    below = jnp.where(first, low if i == 0 else down[i - 1], down[i])
                    above = jnp.where(final, high if i == tiles - 1 else up[i + 1], up[i])
                    beside = cur[p, x, part]
                    if not edge:
                        beside = beside + cur[p, x + 2, part]
                    beside = beside + (below + above)
                    beside = beside + (pltpu.roll(v, 1, 1) + pltpu.roll(v, nz - 1, 1))
                    new = coef[x, part] * v - scale * beside
                    if s == 0:
                        new = 0.5 * new
                    else:
                        new = new - fields[s - 1][p, x + 1, part]
                    if not final_step:
                        fields[s + 1][p, x + 1, part] = new
                        if i == 0:
                            faces[s + 1, 0, p, x] = new[0:1]
                        if i == tiles - 1:
                            faces[s + 1, 1, p, x] = new[ROWS - 1:ROWS]
                    else:
                        last[p, x, part] = new
                    square = square + fold(v * v)
                    cross = cross + fold(new * v)
                return square, cross

            zero = jnp.zeros((ROWS, 128), jnp.float32)
            if final_step:
                square, cross = lax.fori_loop(0, nx - 1, row, (zero, zero), unroll=nx - 1)
                square, cross = row(nx - 1, (square, cross), edge=True)
                for i in range(tiles):
                    part = pl.ds(ROWS * i, ROWS)
                    cross = cross - fold(scale * cur[p, 0, part] * cur[p, 1, part])
            else:
                square, cross = lax.fori_loop(0, nx, row, (zero, zero), unroll=nx)
            acc[0, p] = square
            acc[1, p] = cross
            if s + 1 < STEPS:
                to_low(s + 1, p).start()
                for copy in y_sends(s + 1, p):
                    copy.start()
                if s + 2 < STEPS:
                    to_high(s + 1, p).start()

        for k in range(2):
            total = jnp.sum(jnp.sum(acc[k], axis=1), axis=1, keepdims=True)
            sums = sums + jnp.where(lanes == 2 * s + k, total, 0.0)

    def spread(value, gather, send, recv, me, count, where):
        gather[me] = value
        for offset in range(1, count):
            pltpu.make_async_remote_copy(
                gather.at[me], gather.at[me], send, recv, device_id=where(offset), device_id_type=MESH).start()

    def collect(gather, recv, count):
        arrived(gather.at[pl.ds(0, count - 1)], recv)
        total = gather[0]
        for k in range(1, count):
            total = total + gather[k]
        return total

    def finish(p):
        to_high(STEPS - 1, p).wait_recv()
        for i in range(tiles):
            part = pl.ds(ROWS * i, ROWS)
            last[p, nx - 1, part] = last[p, nx - 1, part] - scale * fields[STEPS - 1][p, nx + 1, part]

    spread(sums, gather_x, gxs_sem, gxr_sem, me_x, count_x, at_x)

    @pl.loop(n_probes - GATE, n_probes)
    def _(p):
        to_high(STEPS - 1, p).start()

    for s in range(STEPS):
        if s + 1 < STEPS:
            arrived(fields[s].at[:, pl.ds(0, 2)], xs_sem.at[s])
        arrived(faces.at[s], ys_sem.at[s])

    pl.loop(0, SPLIT)(finish)
    sums = collect(gather_x, gxr_sem, count_x)
    spread(sums, gather_y, gys_sem, gyr_sem, me_y, count_y, at_y)
    pl.loop(SPLIT, n_probes)(finish)
    sums = collect(gather_y, gyr_sem, count_y)
    mean = sums / jnp.float32(sites)
    start = jnp.where(lax.rem(lanes, 2) == 0, mean[:, 0:1], mean[:, 1:2])
    moments[...] = (2.0 * mean - start)[:, :2 * STEPS]

    arrived(fields[STEPS - 1].at[:, pl.ds(0, 2)], xs_sem.at[STEPS - 1])
    arrived(gather_x.at[pl.ds(0, count_x - 1)], gxs_sem)
    arrived(gather_y.at[pl.ds(0, count_y - 1)], gys_sem)


def local(counts, probes, disorder, spectrum_center, half_width):
    n_probes, nx, ny, nz = probes.shape
    sites = nx * counts[0] * ny * counts[1] * nz
    f32 = jnp.float32
    dma = pltpu.SemaphoreType.DMA
    vmem = pl.BlockSpec(memory_space=pltpu.VMEM)
    smem = pl.BlockSpec(memory_space=pltpu.SMEM)
    hbm = pl.BlockSpec(memory_space=pltpu.HBM)
    return pl.pallas_call(
        functools.partial(kernel, counts, sites),
        out_shape=(
            pltpu.VMEM(probes.shape, f32),
            jax.ShapeDtypeStruct((n_probes, 2 * STEPS), f32),
        ),
        in_specs=[hbm, hbm, smem, smem],
        out_specs=(vmem, vmem),
        scratch_shapes=[pltpu.VMEM((n_probes, nx + 2, ny, nz), f32)] * STEPS + [
            pltpu.VMEM((nx, ny, nz), f32),
            pltpu.VMEM((STEPS, 2, n_probes, nx, 1, nz), f32),
            pltpu.VMEM((STEPS, 2, n_probes, nx, 1, nz), f32),
            pltpu.VMEM((nx, ny, nz), f32),
            pltpu.VMEM((2, n_probes, ROWS, 128), f32),
            pltpu.VMEM((counts[0], n_probes, 128), f32),
            pltpu.VMEM((counts[1], n_probes, 128), f32),
            dma,
            dma,
            dma,
            pltpu.SemaphoreType.REGULAR,
            pltpu.SemaphoreType.REGULAR,
            dma((STEPS,)),
            dma((STEPS,)),
            dma((2, n_probes)),
            dma((2, n_probes)),
            dma((n_probes,)),
            dma,
            dma,
            dma,
            dma,
        ],
        compiler_params=pltpu.CompilerParams(
            collective_id=0, has_side_effects=True, vmem_limit_bytes=46 * 1024 * 1024),
        name="moments",
    )(*(pltpu.with_memory_space_constraint(x, pltpu.HBM) for x in (probes, disorder)),
      spectrum_center, half_width)


def solution(mesh):
    counts = (mesh.shape["gx"], mesh.shape["gy"])
    in_specs = (P(None, "gx", "gy", None), P("gx", "gy", None), P(), P())
    out_specs = (P(None, "gx", "gy", None), P())
    return jax.shard_map(functools.partial(local, counts), mesh=mesh, in_specs=in_specs,
                         out_specs=out_specs, check_vma=False)
```

```python
import functools

import jax
import jax.numpy as jnp
from jax import lax
from jax.experimental import pallas as pl
from jax.experimental.pallas import tpu as pltpu
from jax.sharding import PartitionSpec as P

STEPS = 4
MESH = pl.DeviceIdType.MESH
ROWS = 8
LEAD = (4, 2)
GATES = (4, 5, 8)
SPLIT = 2


def kernel(counts, sites, probes_hbm, disorder_hbm, center, width, last, moments, *scratch):
    fields = scratch[:STEPS]
    (disorder, near, faces, coef, acc, gather_x, gather_y, load_sem, face_sem, energy_sem, up_sem, down_sem,
     round_sem, xs_sem, ys_sem, recv_sem, high_sem, gxs_sem, gxr_sem, gys_sem, gyr_sem) = scratch[STEPS:]
    n_probes, nx, ny, nz = probes_hbm.shape
    tiles = ny // ROWS
    assert 2 * nx % ny == 0 and 2 * STEPS <= nx + 2
    count_x, count_y = counts
    me_x = lax.axis_index("gx")
    me_y = lax.axis_index("gy")

    top = count_x - 1
    gate = jnp.where(me_x == 0, GATES[0], jnp.where(me_x == top, GATES[2], GATES[1]))
    if count_y & (count_y - 1):
        mates = [lax.rem(me_y + k, count_y) for k in range(1, count_y)]
        rounds = 0
    else:
        widths = [1 << k for k in range(count_y.bit_length() - 1)]
        mates = [me_y + w * (1 - 2 * lax.rem(lax.div(me_y, w), 2)) for w in widths]
        rounds = len(widths) - 1

    def at_x(offset):
        return (lax.rem(me_x + offset, count_x), me_y)

    def at_y(offset):
        return (me_x, lax.rem(me_y + offset, count_y))

    def load_face(row):
        return pltpu.make_async_copy(
            probes_hbm.at[:, pl.ds(row, 1)], fields[0].at[:, pl.ds(row + 1, 1)], face_sem)

    def load(p):
        return pltpu.make_async_copy(
            probes_hbm.at[p, pl.ds(1, nx - 2)], fields[0].at[p, pl.ds(2, nx - 2)], load_sem)

    def arrived(ref, sem):
        pltpu.make_async_copy(ref, ref, sem).wait()

    def to_high(s, p):
        final_step = s + 1 == STEPS
        return pltpu.make_async_remote_copy(
            fields[s].at[p, 1], fields[s].at[p, nx + 1], xs_sem,
            high_sem.at[p] if final_step else recv_sem.at[s % 2, p], device_id=at_x(count_x - 1), device_id_type=MESH)

    def to_low(s, p):
        return pltpu.make_async_remote_copy(
            fields[s].at[p, nx], fields[s].at[p, 0], xs_sem, recv_sem.at[s % 2, p],
            device_id=at_x(1), device_id_type=MESH)

    def y_sends(s, p):
        return (
            pltpu.make_async_remote_copy(
                faces.at[s, 0, p], near.at[s, 1, p], ys_sem, recv_sem.at[s % 2, p],
                device_id=at_y(count_y - 1), device_id_type=MESH),
            pltpu.make_async_remote_copy(
                faces.at[s, 1, p], near.at[s, 0, p], ys_sem, recv_sem.at[s % 2, p],
                device_id=at_y(1), device_id_type=MESH),
        )

    barrier = pltpu.get_barrier_semaphore()

    @pl.when(me_x < top)
    def _():
        pl.semaphore_signal(barrier, inc=1, device_id=(me_x + 1, me_y), device_id_type=MESH)

    @pl.when(me_x > 0)
    def _():
        pl.semaphore_signal(barrier, inc=1, device_id=(me_x - 1, me_y), device_id_type=MESH)

    for mate in mates:
        pl.semaphore_signal(barrier, inc=1, device_id=(me_x, mate), device_id_type=MESH)

    for row in (0, nx - 1):
        load_face(row).start()

    @pl.loop(0, n_probes)
    def _(p):
        load(p).start()

    energy = pltpu.make_async_copy(disorder_hbm, disorder, energy_sem)
    energy.start()

    arrived(fields[0].at[:, pl.ds(0, 2)], face_sem)
    pl.semaphore_wait(barrier, len(mates) + (me_x < top).astype(jnp.int32) + (me_x > 0).astype(jnp.int32))

    def greet(k):
        for mate in mates:
            pl.semaphore_signal(round_sem.at[k], inc=1, device_id=(me_x, mate), device_id_type=MESH)

    def take_faces(p):
        def row(x, carry):
            faces[0, 0, p, x] = fields[0][p, x + 1, pl.ds(0, 1)]
            faces[0, 1, p, x] = fields[0][p, x + 1, pl.ds(ny - 1, 1)]
            return carry

        lax.fori_loop(0, nx, row, 0, unroll=4)

    if rounds:
        greet(0)

    @pl.when(me_x == 1)
    def _():
        if count_x > 2:
            pl.semaphore_signal(up_sem, inc=1, device_id=(me_x + 1, me_y), device_id_type=MESH)

    @pl.when(me_x == top - 1)
    def _():
        if count_x > 2:
            pl.semaphore_signal(down_sem, inc=1, device_id=(me_x - 1, me_y), device_id_type=MESH)

    lead = [min(k, n_probes) for k in LEAD]

    @pl.when(me_x == 0)
    def _():
        for p in range(lead[0]):
            to_low(0, p).start()

    @pl.when(me_x == top)
    def _():
        for p in range(lead[1]):
            to_high(0, p).start()

    @pl.when(jnp.logical_and(me_x > 0, me_x < top))
    def _():
        @pl.loop(0, n_probes)
        def _(p):
            to_low(0, p).start()
            to_high(0, p).start()

    arrived(fields[0].at[:, pl.ds(2, nx - 2)], load_sem)
    half = n_probes // 2
    pl.loop(0, half)(take_faces)

    @pl.when(jnp.logical_and(me_x > 0, me_x < top))
    def _():
        @pl.when(me_x > 1)
        def _():
            pl.semaphore_wait(up_sem, 1)
            pl.semaphore_signal(up_sem, inc=1, device_id=(me_x + 1, me_y), device_id_type=MESH)

        @pl.when(me_x < top - 1)
        def _():
            pl.semaphore_wait(down_sem, 1)
            pl.semaphore_signal(down_sem, inc=1, device_id=(me_x - 1, me_y), device_id_type=MESH)

    for k in range(rounds):
        pl.semaphore_wait(round_sem.at[k], len(mates))
        if k + 1 < rounds:
            greet(k + 1)

    @pl.loop(0, half)
    def _(p):
        for copy in y_sends(0, p):
            copy.start()

    def other_sends(lead, adjacent, wrapped, proof):
        if count_x > 2:
            pl.semaphore_wait(proof, 1)
        for p in range(lead, n_probes):
            wrapped(0, p - lead).start()
            adjacent(0, p).start()
        for p in range(n_probes - lead, n_probes):
            wrapped(0, p).start()

    @pl.when(me_x == 0)
    def _():
        other_sends(lead[0], to_low, to_high, down_sem)

    @pl.when(me_x == top)
    def _():
        other_sends(lead[1], to_high, to_low, up_sem)

    @pl.loop(half, n_probes)
    def _(p):
        take_faces(p)
        for copy in y_sends(0, p):
            copy.start()

    scale = 2.0 / jnp.full((ROWS, nz), width[0], jnp.float32)
    middle = center[0]
    energy.wait()

    @pl.loop(0, nx)
    def _(x):
        for i in range(tiles):
            part = pl.ds(ROWS * i, ROWS)
            coef[x, part] = (disorder[x, part] - middle) * scale

    sub = lax.broadcasted_iota(jnp.int32, (ROWS, nz), 0)
    first = sub == 0
    final = sub == ROWS - 1
    lanes = lax.broadcasted_iota(jnp.int32, (n_probes, 128), 1)
    sums = jnp.zeros((n_probes, 128), jnp.float32)

    def fold(v):
        parts = [v[:, 128 * j:128 * (j + 1)] for j in range(nz // 128)]
        while len(parts) > 1:
            parts = [a + b for a, b in zip(parts[::2], parts[1::2])] + (
                [parts[-1]] if len(parts) % 2 else [])
        return parts[0]

    for s in range(STEPS):
        cur = fields[s]
        final_step = s + 1 == STEPS

        @pl.loop(0, n_probes)
        def _(p):
            arrived(cur.at[p, pl.ds(0, 2 * nx // ny + (1 if final_step else 2))], recv_sem.at[s % 2, p])
            if final_step:
                @pl.when(p >= gate)
                def _():
                    to_high(s, p - gate).start()

            def row(x, carry, edge=False):
                square, cross = carry
                low = jnp.broadcast_to(near[s, 0, p, x], (ROWS, nz))
                high = jnp.broadcast_to(near[s, 1, p, x], (ROWS, nz))
                here = [cur[p, x + 1, pl.ds(ROWS * i, ROWS)] for i in range(tiles)]
                down = [pltpu.roll(v, 1, 0) for v in here]
                up = [pltpu.roll(v, ROWS - 1, 0) for v in here]
                for i in range(tiles):
                    part = pl.ds(ROWS * i, ROWS)
                    v = here[i]
                    below = jnp.where(first, low if i == 0 else down[i - 1], down[i])
                    above = jnp.where(final, high if i == tiles - 1 else up[i + 1], up[i])
                    beside = cur[p, x, part]
                    if not edge:
                        beside = beside + cur[p, x + 2, part]
                    beside = beside + (below + above)
                    beside = beside + (pltpu.roll(v, 1, 1) + pltpu.roll(v, nz - 1, 1))
                    new = coef[x, part] * v - scale * beside
                    if s == 0:
                        new = 0.5 * new
                    else:
                        new = new - fields[s - 1][p, x + 1, part]
                    if not final_step:
                        fields[s + 1][p, x + 1, part] = new
                        if i == 0:
                            faces[s + 1, 0, p, x] = new[0:1]
                        if i == tiles - 1:
                            faces[s + 1, 1, p, x] = new[ROWS - 1:ROWS]
                    else:
                        last[p, x, part] = new
                    square = square + fold(v * v)
                    cross = cross + fold(new * v)
                return square, cross

            zero = jnp.zeros((ROWS, 128), jnp.float32)
            if final_step:
                square, cross = lax.fori_loop(0, nx - 1, row, (zero, zero), unroll=nx - 1)
                square, cross = row(nx - 1, (square, cross), edge=True)
                for i in range(tiles):
                    part = pl.ds(ROWS * i, ROWS)
                    cross = cross - fold(scale * cur[p, 0, part] * cur[p, 1, part])
            else:
                square, cross = lax.fori_loop(0, nx, row, (zero, zero), unroll=nx)
            acc[0, p] = square
            acc[1, p] = cross
            if s + 1 < STEPS:
                to_low(s + 1, p).start()
                for copy in y_sends(s + 1, p):
                    copy.start()
                if s + 2 < STEPS:
                    to_high(s + 1, p).start()

        for k in range(2):
            total = jnp.sum(jnp.sum(acc[k], axis=1), axis=1, keepdims=True)
            sums = sums + jnp.where(lanes == 2 * s + k, total, 0.0)

    def spread(value, gather, send, recv, me, count, where):
        gather[me] = value
        for offset in range(1, count):
            pltpu.make_async_remote_copy(
                gather.at[me], gather.at[me], send, recv, device_id=where(offset), device_id_type=MESH).start()

    def collect(gather, recv, count):
        arrived(gather.at[pl.ds(0, count - 1)], recv)
        total = gather[0]
        for k in range(1, count):
            total = total + gather[k]
        return total

    def finish(p):
        to_high(STEPS - 1, p).wait_recv()
        for i in range(tiles):
            part = pl.ds(ROWS * i, ROWS)
            last[p, nx - 1, part] = last[p, nx - 1, part] - scale * fields[STEPS - 1][p, nx + 1, part]

    spread(sums, gather_x, gxs_sem, gxr_sem, me_x, count_x, at_x)

    @pl.loop(n_probes - gate, n_probes)
    def _(p):
        to_high(STEPS - 1, p).start()

    pl.loop(0, SPLIT)(finish)
    sums = collect(gather_x, gxr_sem, count_x)
    spread(sums, gather_y, gys_sem, gyr_sem, me_y, count_y, at_y)
    pl.loop(SPLIT, n_probes)(finish)
    sums = collect(gather_y, gyr_sem, count_y)
    mean = sums / jnp.float32(sites)
    start = jnp.where(lax.rem(lanes, 2) == 0, mean[:, 0:1], mean[:, 1:2])
    moments[...] = (2.0 * mean - start)[:, :2 * STEPS]

    arrived(fields[0].at[:, pl.ds(0, 2 * STEPS)], xs_sem)
    arrived(faces, ys_sem)
    arrived(gather_x.at[pl.ds(0, count_x - 1)], gxs_sem)
    arrived(gather_y.at[pl.ds(0, count_y - 1)], gys_sem)


def write_out(last, moments, last_hbm, moments_hbm, last_sem, moments_sem):
    small = pltpu.make_async_copy(moments, moments_hbm, moments_sem)
    small.start()
    for p in range(last.shape[0]):
        pltpu.make_async_copy(last.at[p], last_hbm.at[p], last_sem).start()
    small.wait()
    pltpu.make_async_copy(last, last_hbm, last_sem).wait()


def local(counts, probes, disorder, spectrum_center, half_width):
    n_probes, nx, ny, nz = probes.shape
    sites = nx * counts[0] * ny * counts[1] * nz
    f32 = jnp.float32
    dma = pltpu.SemaphoreType.DMA
    vmem = pl.BlockSpec(memory_space=pltpu.VMEM)
    smem = pl.BlockSpec(memory_space=pltpu.SMEM)
    hbm = pl.BlockSpec(memory_space=pltpu.HBM)
    held = pl.pallas_call(
        functools.partial(kernel, counts, sites),
        out_shape=(
            pltpu.VMEM(probes.shape, f32),
            jax.ShapeDtypeStruct((n_probes, 2 * STEPS), f32),
        ),
        in_specs=[hbm, hbm, smem, smem],
        out_specs=(vmem, vmem),
        scratch_shapes=[pltpu.VMEM((n_probes, nx + 2, ny, nz), f32)] * STEPS + [
            pltpu.VMEM((nx, ny, nz), f32),
            pltpu.VMEM((STEPS, 2, n_probes, nx, 1, nz), f32),
            pltpu.VMEM((STEPS, 2, n_probes, nx, 1, nz), f32),
            pltpu.VMEM((nx, ny, nz), f32),
            pltpu.VMEM((2, n_probes, ROWS, 128), f32),
            pltpu.VMEM((counts[0], n_probes, 128), f32),
            pltpu.VMEM((counts[1], n_probes, 128), f32),
            dma,
            dma,
            dma,
            pltpu.SemaphoreType.REGULAR,
            pltpu.SemaphoreType.REGULAR,
            pltpu.SemaphoreType.REGULAR((max(counts[1].bit_length() - 2, 1),)),
            dma,
            dma,
            dma((2, n_probes)),
            dma((n_probes,)),
            dma,
            dma,
            dma,
            dma,
        ],
        compiler_params=pltpu.CompilerParams(
            collective_id=0, has_side_effects=True, vmem_limit_bytes=32 * 1024 * 1024),
        name="moments",
    )(*(pltpu.with_memory_space_constraint(x, pltpu.HBM) for x in (probes, disorder)),
      spectrum_center, half_width)
    return pl.pallas_call(
        write_out,
        out_shape=(jax.ShapeDtypeStruct(probes.shape, f32), jax.ShapeDtypeStruct((n_probes, 2 * STEPS), f32)),
        in_specs=[vmem] * 2,
        out_specs=(hbm,) * 2,
        scratch_shapes=[dma, dma],
        compiler_params=pltpu.CompilerParams(vmem_limit_bytes=8 * 1024 * 1024),
        name="write_out",
    )(*(pltpu.with_memory_space_constraint(x, pltpu.VMEM) for x in held))


def solution(mesh):
    counts = (mesh.shape["gx"], mesh.shape["gy"])
    in_specs = (P(None, "gx", "gy", None), P("gx", "gy", None), P(), P())
    out_specs = (P(None, "gx", "gy", None), P())
    return jax.shard_map(functools.partial(local, counts), mesh=mesh, in_specs=in_specs,
                         out_specs=out_specs, check_vma=False)
```

```python
import functools

import jax
import jax.numpy as jnp
from jax import lax
from jax.experimental import pallas as pl
from jax.experimental.pallas import tpu as pltpu
from jax.sharding import PartitionSpec as P

STEPS = 4
MESH = pl.DeviceIdType.MESH
ROWS = 8
LEAD = (5, 4)
GATES = (4, 5, 6, 8)
SPLIT = 2


def kernel(counts, sites, probes_hbm, disorder_hbm, center, width, last, moments, *scratch):
    fields = scratch[:STEPS]
    (disorder, near, faces, coef, acc, gather_x, gather_y, load_sem, face_sem, energy_sem, up_sem, down_sem,
     round_sem, xs_sem, ys_sem, recv_sem, high_sem, gxs_sem, gxr_sem, gys_sem, gyr_sem) = scratch[STEPS:]
    n_probes, nx, ny, nz = probes_hbm.shape
    tiles = ny // ROWS
    assert 2 * nx % ny == 0 and 2 * STEPS <= nx + 2
    count_x, count_y = counts
    me_x = lax.axis_index("gx")
    me_y = lax.axis_index("gy")

    top = count_x - 1
    gate = jnp.where(me_x == 0, GATES[0], jnp.where(me_x == 1, GATES[1], jnp.where(me_x < top, GATES[2], GATES[3])))
    if count_y & (count_y - 1):
        mates = [lax.rem(me_y + k, count_y) for k in range(1, count_y)]
        rounds = 0
    else:
        widths = [1 << k for k in range(count_y.bit_length() - 1)]
        mates = [me_y + w * (1 - 2 * lax.rem(lax.div(me_y, w), 2)) for w in widths]
        rounds = len(widths) - 1

    def at_x(offset):
        return (lax.rem(me_x + offset, count_x), me_y)

    def at_y(offset):
        return (me_x, lax.rem(me_y + offset, count_y))

    def load_face(row):
        return pltpu.make_async_copy(
            probes_hbm.at[:, pl.ds(row, 1)], fields[0].at[:, pl.ds(row + 1, 1)], face_sem)

    def load(p):
        return pltpu.make_async_copy(
            probes_hbm.at[p, pl.ds(1, nx - 2)], fields[0].at[p, pl.ds(2, nx - 2)], load_sem)

    def arrived(ref, sem):
        pltpu.make_async_copy(ref, ref, sem).wait()

    def to_high(s, p):
        final_step = s + 1 == STEPS
        return pltpu.make_async_remote_copy(
            fields[s].at[p, 1], fields[s].at[p, nx + 1], xs_sem,
            high_sem.at[p] if final_step else recv_sem.at[s % 2, p], device_id=at_x(count_x - 1), device_id_type=MESH)

    def to_low(s, p):
        return pltpu.make_async_remote_copy(
            fields[s].at[p, nx], fields[s].at[p, 0], xs_sem, recv_sem.at[s % 2, p],
            device_id=at_x(1), device_id_type=MESH)

    def y_sends(s, p):
        return (
            pltpu.make_async_remote_copy(
                faces.at[s, 0, p], near.at[s, 1, p], ys_sem, recv_sem.at[s % 2, p],
                device_id=at_y(count_y - 1), device_id_type=MESH),
            pltpu.make_async_remote_copy(
                faces.at[s, 1, p], near.at[s, 0, p], ys_sem, recv_sem.at[s % 2, p],
                device_id=at_y(1), device_id_type=MESH),
        )

    barrier = pltpu.get_barrier_semaphore()

    @pl.when(me_x < top)
    def _():
        pl.semaphore_signal(barrier, inc=1, device_id=(me_x + 1, me_y), device_id_type=MESH)

    @pl.when(me_x > 0)
    def _():
        pl.semaphore_signal(barrier, inc=1, device_id=(me_x - 1, me_y), device_id_type=MESH)

    for mate in mates:
        pl.semaphore_signal(barrier, inc=1, device_id=(me_x, mate), device_id_type=MESH)

    for row in (0, nx - 1):
        load_face(row).start()

    @pl.loop(0, n_probes)
    def _(p):
        load(p).start()

    energy = pltpu.make_async_copy(disorder_hbm, disorder, energy_sem)
    energy.start()

    arrived(fields[0].at[:, pl.ds(0, 2)], face_sem)
    pl.semaphore_wait(barrier, len(mates) + (me_x < top).astype(jnp.int32) + (me_x > 0).astype(jnp.int32))

    def greet(k):
        for mate in mates:
            pl.semaphore_signal(round_sem.at[k], inc=1, device_id=(me_x, mate), device_id_type=MESH)

    def take_faces(p):
        def row(x, carry):
            faces[0, 0, p, x] = fields[0][p, x + 1, pl.ds(0, 1)]
            faces[0, 1, p, x] = fields[0][p, x + 1, pl.ds(ny - 1, 1)]
            return carry

        lax.fori_loop(0, nx, row, 0, unroll=4)

    if rounds:
        greet(0)

    @pl.when(me_x == 1)
    def _():
        if count_x > 2:
            pl.semaphore_signal(up_sem, inc=1, device_id=(me_x + 1, me_y), device_id_type=MESH)

    @pl.when(me_x == top - 1)
    def _():
        if count_x > 2:
            pl.semaphore_signal(down_sem, inc=1, device_id=(me_x - 1, me_y), device_id_type=MESH)

    lead = [min(k, n_probes) for k in LEAD]

    @pl.when(me_x == 0)
    def _():
        for p in range(lead[0]):
            to_low(0, p).start()

    @pl.when(me_x == top)
    def _():
        for p in range(lead[1]):
            to_high(0, p).start()

    @pl.when(jnp.logical_and(me_x > 0, me_x < top))
    def _():
        @pl.loop(0, n_probes)
        def _(p):
            to_low(0, p).start()
            to_high(0, p).start()

    arrived(fields[0].at[:, pl.ds(2, nx - 2)], load_sem)
    pl.loop(0, n_probes)(take_faces)

    def other_sends(lead, adjacent, wrapped, proof):
        if count_x > 2:
            pl.semaphore_wait(proof, 1)
        for p in range(lead, n_probes):
            wrapped(0, p - lead).start()
            adjacent(0, p).start()
        for p in range(n_probes - lead, n_probes):
            wrapped(0, p).start()

    def pass_on():
        @pl.when(jnp.logical_and(me_x > 1, me_x < top))
        def _():
            pl.semaphore_wait(up_sem, 1)
            pl.semaphore_signal(up_sem, inc=1, device_id=(me_x + 1, me_y), device_id_type=MESH)

        @pl.when(jnp.logical_and(me_x > 0, me_x < top - 1))
        def _():
            pl.semaphore_wait(down_sem, 1)
            pl.semaphore_signal(down_sem, inc=1, device_id=(me_x - 1, me_y), device_id_type=MESH)

        @pl.when(me_x == 0)
        def _():
            other_sends(lead[0], to_low, to_high, down_sem)

        @pl.when(me_x == top)
        def _():
            other_sends(lead[1], to_high, to_low, up_sem)

    for k in range(rounds):
        pl.semaphore_wait(round_sem.at[k], len(mates))
        if k + 1 < rounds:
            greet(k + 1)
        if k == 0:
            pass_on()
    if not rounds:
        pass_on()

    @pl.loop(0, n_probes)
    def _(p):
        for copy in y_sends(0, p):
            copy.start()

    scale = 2.0 / jnp.full((ROWS, nz), width[0], jnp.float32)
    middle = center[0]
    energy.wait()

    @pl.loop(0, nx)
    def _(x):
        for i in range(tiles):
            part = pl.ds(ROWS * i, ROWS)
            coef[x, part] = (disorder[x, part] - middle) * scale

    sub = lax.broadcasted_iota(jnp.int32, (ROWS, nz), 0)
    first = sub == 0
    final = sub == ROWS - 1
    lanes = lax.broadcasted_iota(jnp.int32, (n_probes, 128), 1)
    sums = jnp.zeros((n_probes, 128), jnp.float32)

    def fold(v):
        parts = [v[:, 128 * j:128 * (j + 1)] for j in range(nz // 128)]
        while len(parts) > 1:
            parts = [a + b for a, b in zip(parts[::2], parts[1::2])] + (
                [parts[-1]] if len(parts) % 2 else [])
        return parts[0]

    for s in range(STEPS):
        cur = fields[s]
        final_step = s + 1 == STEPS

        @pl.loop(0, n_probes)
        def _(p):
            arrived(cur.at[p, pl.ds(0, 2 * nx // ny + (1 if final_step else 2))], recv_sem.at[s % 2, p])
            if final_step:
                @pl.when(p >= gate)
                def _():
                    to_high(s, p - gate).start()

            def row(x, carry, edge=False):
                square, cross = carry
                low = jnp.broadcast_to(near[s, 0, p, x], (ROWS, nz))
                high = jnp.broadcast_to(near[s, 1, p, x], (ROWS, nz))
                here = [cur[p, x + 1, pl.ds(ROWS * i, ROWS)] for i in range(tiles)]
                down = [pltpu.roll(v, 1, 0) for v in here]
                up = [pltpu.roll(v, ROWS - 1, 0) for v in here]
                for i in range(tiles):
                    part = pl.ds(ROWS * i, ROWS)
                    v = here[i]
                    below = jnp.where(first, low if i == 0 else down[i - 1], down[i])
                    above = jnp.where(final, high if i == tiles - 1 else up[i + 1], up[i])
                    beside = cur[p, x, part]
                    if not edge:
                        beside = beside + cur[p, x + 2, part]
                    beside = beside + (below + above)
                    beside = beside + (pltpu.roll(v, 1, 1) + pltpu.roll(v, nz - 1, 1))
                    new = coef[x, part] * v - scale * beside
                    if s == 0:
                        new = 0.5 * new
                    else:
                        new = new - fields[s - 1][p, x + 1, part]
                    if not final_step:
                        fields[s + 1][p, x + 1, part] = new
                        if i == 0:
                            faces[s + 1, 0, p, x] = new[0:1]
                        if i == tiles - 1:
                            faces[s + 1, 1, p, x] = new[ROWS - 1:ROWS]
                    else:
                        last[p, x, part] = new
                    square = square + fold(v * v)
                    cross = cross + fold(new * v)
                return square, cross

            zero = jnp.zeros((ROWS, 128), jnp.float32)
            if final_step:
                square, cross = lax.fori_loop(0, nx - 1, row, (zero, zero), unroll=nx - 1)
                square, cross = row(nx - 1, (square, cross), edge=True)
                for i in range(tiles):
                    part = pl.ds(ROWS * i, ROWS)
                    cross = cross - fold(scale * cur[p, 0, part] * cur[p, 1, part])
            else:
                square, cross = lax.fori_loop(0, nx, row, (zero, zero), unroll=nx)
            acc[0, p] = square
            acc[1, p] = cross
            if s + 1 < STEPS:
                to_low(s + 1, p).start()
                for copy in y_sends(s + 1, p):
                    copy.start()
                if s + 2 < STEPS:
                    to_high(s + 1, p).start()

        for k in range(2):
            total = jnp.sum(jnp.sum(acc[k], axis=1), axis=1, keepdims=True)
            sums = sums + jnp.where(lanes == 2 * s + k, total, 0.0)

    def spread(value, gather, send, recv, me, count, where):
        gather[me] = value
        for offset in range(1, count):
            pltpu.make_async_remote_copy(
                gather.at[me], gather.at[me], send, recv, device_id=where(offset), device_id_type=MESH).start()

    def collect(gather, recv, count):
        arrived(gather.at[pl.ds(0, count - 1)], recv)
        total = gather[0]
        for k in range(1, count):
            total = total + gather[k]
        return total

    def finish(p):
        to_high(STEPS - 1, p).wait_recv()
        for i in range(tiles):
            part = pl.ds(ROWS * i, ROWS)
            last[p, nx - 1, part] = last[p, nx - 1, part] - scale * fields[STEPS - 1][p, nx + 1, part]

    spread(sums, gather_x, gxs_sem, gxr_sem, me_x, count_x, at_x)

    @pl.loop(n_probes - gate, n_probes)
    def _(p):
        to_high(STEPS - 1, p).start()

    pl.loop(0, SPLIT)(finish)
    sums = collect(gather_x, gxr_sem, count_x)
    spread(sums, gather_y, gys_sem, gyr_sem, me_y, count_y, at_y)
    pl.loop(SPLIT, n_probes)(finish)
    sums = collect(gather_y, gyr_sem, count_y)
    mean = sums / jnp.float32(sites)
    start = jnp.where(lax.rem(lanes, 2) == 0, mean[:, 0:1], mean[:, 1:2])
    moments[...] = (2.0 * mean - start)[:, :2 * STEPS]

    arrived(fields[0].at[:, pl.ds(0, 2 * STEPS)], xs_sem)
    arrived(faces, ys_sem)
    arrived(gather_x.at[pl.ds(0, count_x - 1)], gxs_sem)
    arrived(gather_y.at[pl.ds(0, count_y - 1)], gys_sem)


def write_out(last, moments, last_hbm, moments_hbm, last_sem, moments_sem):
    small = pltpu.make_async_copy(moments, moments_hbm, moments_sem)
    small.start()
    for p in range(last.shape[0]):
        pltpu.make_async_copy(last.at[p], last_hbm.at[p], last_sem).start()
    small.wait()
    pltpu.make_async_copy(last, last_hbm, last_sem).wait()


def local(counts, probes, disorder, spectrum_center, half_width):
    n_probes, nx, ny, nz = probes.shape
    sites = nx * counts[0] * ny * counts[1] * nz
    f32 = jnp.float32
    dma = pltpu.SemaphoreType.DMA
    vmem = pl.BlockSpec(memory_space=pltpu.VMEM)
    smem = pl.BlockSpec(memory_space=pltpu.SMEM)
    hbm = pl.BlockSpec(memory_space=pltpu.HBM)
    held = pl.pallas_call(
        functools.partial(kernel, counts, sites),
        out_shape=(
            pltpu.VMEM(probes.shape, f32),
            jax.ShapeDtypeStruct((n_probes, 2 * STEPS), f32),
        ),
        in_specs=[hbm, hbm, smem, smem],
        out_specs=(vmem, vmem),
        scratch_shapes=[pltpu.VMEM((n_probes, nx + 2, ny, nz), f32)] * STEPS + [
            pltpu.VMEM((nx, ny, nz), f32),
            pltpu.VMEM((STEPS, 2, n_probes, nx, 1, nz), f32),
            pltpu.VMEM((STEPS, 2, n_probes, nx, 1, nz), f32),
            pltpu.VMEM((nx, ny, nz), f32),
            pltpu.VMEM((2, n_probes, ROWS, 128), f32),
            pltpu.VMEM((counts[0], n_probes, 128), f32),
            pltpu.VMEM((counts[1], n_probes, 128), f32),
            dma,
            dma,
            dma,
            pltpu.SemaphoreType.REGULAR,
            pltpu.SemaphoreType.REGULAR,
            pltpu.SemaphoreType.REGULAR((max(counts[1].bit_length() - 2, 1),)),
            dma,
            dma,
            dma((2, n_probes)),
            dma((n_probes,)),
            dma,
            dma,
            dma,
            dma,
        ],
        compiler_params=pltpu.CompilerParams(
            collective_id=0, has_side_effects=True, vmem_limit_bytes=32 * 1024 * 1024),
        name="moments",
    )(*(pltpu.with_memory_space_constraint(x, pltpu.HBM) for x in (probes, disorder)),
      spectrum_center, half_width)
    return pl.pallas_call(
        write_out,
        out_shape=(jax.ShapeDtypeStruct(probes.shape, f32), jax.ShapeDtypeStruct((n_probes, 2 * STEPS), f32)),
        in_specs=[vmem] * 2,
        out_specs=(hbm,) * 2,
        scratch_shapes=[dma, dma],
        compiler_params=pltpu.CompilerParams(vmem_limit_bytes=8 * 1024 * 1024),
        name="write_out",
    )(*(pltpu.with_memory_space_constraint(x, pltpu.VMEM) for x in held))


def solution(mesh):
    counts = (mesh.shape["gx"], mesh.shape["gy"])
    in_specs = (P(None, "gx", "gy", None), P("gx", "gy", None), P(), P())
    out_specs = (P(None, "gx", "gy", None), P())
    return jax.shard_map(functools.partial(local, counts), mesh=mesh, in_specs=in_specs,
                         out_specs=out_specs, check_vma=False)
```

```python
import functools

import jax
import jax.numpy as jnp
from jax import lax
from jax.experimental import pallas as pl
from jax.experimental.pallas import tpu as pltpu
from jax.sharding import PartitionSpec as P

STEPS = 4
MESH = pl.DeviceIdType.MESH
ROWS = 8
LEAD = (5, 4)
GATES = (4, 5, 6, 8)
SPLIT = 2


def kernel(counts, sites, probes_hbm, disorder_hbm, center, width, last, moments, *scratch):
    fields = scratch[:STEPS]
    (disorder, near, faces, coef, acc, gather_x, gather_y, load_sem, face_sem, energy_sem, up_sem, down_sem,
     round_sem, xs_sem, ys_sem, recv_sem, low_sem, high_sem, gxs_sem, gxr_sem, gys_sem, gyr_sem) = scratch[STEPS:]
    n_probes, nx, ny, nz = probes_hbm.shape
    tiles = ny // ROWS
    assert 2 * nx % ny == 0 and 2 * STEPS <= nx + 2 and 2 * STEPS * n_probes <= 128
    count_x, count_y = counts
    me_x = lax.axis_index("gx")
    me_y = lax.axis_index("gy")

    top = count_x - 1
    gate = jnp.where(me_x == 0, GATES[0], jnp.where(me_x == 1, GATES[1], jnp.where(me_x < top, GATES[2], GATES[3])))
    if count_y & (count_y - 1):
        mates = [lax.rem(me_y + k, count_y) for k in range(1, count_y)]
        rounds = 0
    else:
        widths = [1 << k for k in range(count_y.bit_length() - 1)]
        mates = [me_y + w * (1 - 2 * lax.rem(lax.div(me_y, w), 2)) for w in widths]
        rounds = len(widths) - 1

    def at_x(offset):
        return (lax.rem(me_x + offset, count_x), me_y)

    def at_y(offset):
        return (me_x, lax.rem(me_y + offset, count_y))

    def load_face(row):
        return pltpu.make_async_copy(
            probes_hbm.at[:, pl.ds(row, 1)], fields[0].at[:, pl.ds(row + 1, 1)], face_sem)

    def load(p):
        return pltpu.make_async_copy(
            probes_hbm.at[p, pl.ds(1, nx - 2)], fields[0].at[p, pl.ds(2, nx - 2)], load_sem)

    def arrived(ref, sem):
        pltpu.make_async_copy(ref, ref, sem).wait()

    def to_high(s, p):
        final_step = s + 1 == STEPS
        return pltpu.make_async_remote_copy(
            fields[s].at[p, 1], fields[s].at[p, nx + 1], xs_sem,
            high_sem.at[p] if final_step else recv_sem.at[s % 2, p], device_id=at_x(count_x - 1), device_id_type=MESH)

    def to_low(s, p):
        return pltpu.make_async_remote_copy(
            fields[s].at[p, nx], fields[s].at[p, 0], xs_sem,
            low_sem.at[p] if s + 1 == STEPS else recv_sem.at[s % 2, p], device_id=at_x(1), device_id_type=MESH)

    def y_sends(s, p):
        return (
            pltpu.make_async_remote_copy(
                faces.at[s, 0, p], near.at[s, 1, p], ys_sem, recv_sem.at[s % 2, p],
                device_id=at_y(count_y - 1), device_id_type=MESH),
            pltpu.make_async_remote_copy(
                faces.at[s, 1, p], near.at[s, 0, p], ys_sem, recv_sem.at[s % 2, p],
                device_id=at_y(1), device_id_type=MESH),
        )

    barrier = pltpu.get_barrier_semaphore()

    @pl.when(me_x < top)
    def _():
        pl.semaphore_signal(barrier, inc=1, device_id=(me_x + 1, me_y), device_id_type=MESH)

    @pl.when(me_x > 0)
    def _():
        pl.semaphore_signal(barrier, inc=1, device_id=(me_x - 1, me_y), device_id_type=MESH)

    for mate in mates:
        pl.semaphore_signal(barrier, inc=1, device_id=(me_x, mate), device_id_type=MESH)

    for row in (0, nx - 1):
        load_face(row).start()

    @pl.loop(0, n_probes)
    def _(p):
        load(p).start()

    energy = pltpu.make_async_copy(disorder_hbm, disorder, energy_sem)
    energy.start()

    arrived(fields[0].at[:, pl.ds(0, 2)], face_sem)
    pl.semaphore_wait(barrier, len(mates) + (me_x < top).astype(jnp.int32) + (me_x > 0).astype(jnp.int32))

    def greet(k):
        for mate in mates:
            pl.semaphore_signal(round_sem.at[k], inc=1, device_id=(me_x, mate), device_id_type=MESH)

    def take_faces(p):
        def row(x, carry):
            faces[0, 0, p, x] = fields[0][p, x + 1, pl.ds(0, 1)]
            faces[0, 1, p, x] = fields[0][p, x + 1, pl.ds(ny - 1, 1)]
            return carry

        lax.fori_loop(0, nx, row, 0, unroll=4)

    if rounds:
        greet(0)

    @pl.when(me_x == 1)
    def _():
        if count_x > 2:
            pl.semaphore_signal(up_sem, inc=1, device_id=(me_x + 1, me_y), device_id_type=MESH)

    @pl.when(me_x == top - 1)
    def _():
        if count_x > 2:
            pl.semaphore_signal(down_sem, inc=1, device_id=(me_x - 1, me_y), device_id_type=MESH)

    lead = [min(k, n_probes) for k in LEAD]

    @pl.when(me_x == 0)
    def _():
        for p in range(lead[0]):
            to_low(0, p).start()

    @pl.when(me_x == top)
    def _():
        for p in range(lead[1]):
            to_high(0, p).start()

    @pl.when(jnp.logical_and(me_x > 0, me_x < top))
    def _():
        @pl.loop(0, n_probes)
        def _(p):
            to_low(0, p).start()
            to_high(0, p).start()

    arrived(fields[0].at[:, pl.ds(2, nx - 2)], load_sem)
    pl.loop(0, n_probes)(take_faces)

    def other_sends(lead, adjacent, wrapped, proof):
        if count_x > 2:
            pl.semaphore_wait(proof, 1)
        for p in range(lead, n_probes):
            wrapped(0, p - lead).start()
            adjacent(0, p).start()
        for p in range(n_probes - lead, n_probes):
            wrapped(0, p).start()

    def pass_on():
        @pl.when(jnp.logical_and(me_x > 1, me_x < top))
        def _():
            pl.semaphore_wait(up_sem, 1)
            pl.semaphore_signal(up_sem, inc=1, device_id=(me_x + 1, me_y), device_id_type=MESH)

        @pl.when(jnp.logical_and(me_x > 0, me_x < top - 1))
        def _():
            pl.semaphore_wait(down_sem, 1)
            pl.semaphore_signal(down_sem, inc=1, device_id=(me_x - 1, me_y), device_id_type=MESH)

        @pl.when(me_x == 0)
        def _():
            other_sends(lead[0], to_low, to_high, down_sem)

        @pl.when(me_x == top)
        def _():
            other_sends(lead[1], to_high, to_low, up_sem)

    for k in range(rounds):
        pl.semaphore_wait(round_sem.at[k], len(mates))
        if k + 1 < rounds:
            greet(k + 1)
        if k == 0:
            pass_on()
    if not rounds:
        pass_on()

    @pl.loop(0, n_probes)
    def _(p):
        for copy in y_sends(0, p):
            copy.start()

    scale = 2.0 / jnp.full((ROWS, nz), width[0], jnp.float32)
    middle = center[0]
    energy.wait()

    @pl.loop(0, nx)
    def _(x):
        for i in range(tiles):
            part = pl.ds(ROWS * i, ROWS)
            coef[x, part] = (disorder[x, part] - middle) * scale

    sub = lax.broadcasted_iota(jnp.int32, (ROWS, nz), 0)
    first = sub == 0
    final = sub == ROWS - 1
    lanes = lax.broadcasted_iota(jnp.int32, (n_probes, 128), 1)
    which = lax.broadcasted_iota(jnp.int32, (n_probes, 128), 0)
    sums = jnp.zeros((n_probes, 128), jnp.float32)

    def fold(v):
        parts = [v[:, 128 * j:128 * (j + 1)] for j in range(nz // 128)]
        while len(parts) > 1:
            parts = [a + b for a, b in zip(parts[::2], parts[1::2])] + (
                [parts[-1]] if len(parts) % 2 else [])
        return parts[0]

    for s in range(STEPS):
        cur = fields[s]
        final_step = s + 1 == STEPS

        @pl.loop(0, n_probes)
        def _(p):
            if final_step:
                arrived(near.at[s, :, p], recv_sem.at[s % 2, p])
            else:
                arrived(cur.at[p, pl.ds(0, 2 * nx // ny + 2)], recv_sem.at[s % 2, p])

            def row(x, carry, below_x=True, above_x=True):
                square, cross = carry
                low = jnp.broadcast_to(near[s, 0, p, x], (ROWS, nz))
                high = jnp.broadcast_to(near[s, 1, p, x], (ROWS, nz))
                here = [cur[p, x + 1, pl.ds(ROWS * i, ROWS)] for i in range(tiles)]
                down = [pltpu.roll(v, 1, 0) for v in here]
                up = [pltpu.roll(v, ROWS - 1, 0) for v in here]
                for i in range(tiles):
                    part = pl.ds(ROWS * i, ROWS)
                    v = here[i]
                    below = jnp.where(first, low if i == 0 else down[i - 1], down[i])
                    above = jnp.where(final, high if i == tiles - 1 else up[i + 1], up[i])
                    beside = below + above
                    if below_x:
                        beside = beside + cur[p, x, part]
                    if above_x:
                        beside = beside + cur[p, x + 2, part]
                    beside = beside + (pltpu.roll(v, 1, 1) + pltpu.roll(v, nz - 1, 1))
                    new = coef[x, part] * v - scale * beside
                    if s == 0:
                        new = 0.5 * new
                    else:
                        new = new - fields[s - 1][p, x + 1, part]
                    if not final_step:
                        fields[s + 1][p, x + 1, part] = new
                        if i == 0:
                            faces[s + 1, 0, p, x] = new[0:1]
                        if i == tiles - 1:
                            faces[s + 1, 1, p, x] = new[ROWS - 1:ROWS]
                    else:
                        last[p, x, part] = new
                    square = square + fold(v * v)
                    cross = cross + fold(new * v)
                return square, cross

            zero = jnp.zeros((ROWS, 128), jnp.float32)
            if final_step:
                sums_p = row(0, (zero, zero), below_x=False)
                sums_p = lax.fori_loop(1, nx - 1, row, sums_p, unroll=nx - 2)
                square, cross = row(nx - 1, sums_p, above_x=False)
            else:
                square, cross = lax.fori_loop(0, nx, row, (zero, zero), unroll=nx)
            acc[0, p] = square
            acc[1, p] = cross
            if s + 1 < STEPS:
                to_low(s + 1, p).start()
                for copy in y_sends(s + 1, p):
                    copy.start()
                if s + 2 < STEPS:
                    to_high(s + 1, p).start()

        if final_step:
            @pl.loop(0, n_probes)
            def _(p):
                to_low(s, p).wait_recv()

                @pl.when(p >= gate)
                def _():
                    to_high(s, p - gate).start()

                bond = jnp.zeros((ROWS, 128), jnp.float32)
                for i in range(tiles):
                    part = pl.ds(ROWS * i, ROWS)
                    below = scale * cur[p, 0, part]
                    last[p, 0, part] = last[p, 0, part] - below
                    bond = bond + fold(below * cur[p, 1, part])
                acc[1, p] = acc[1, p] - 2.0 * bond

        for k in range(2):
            total = jnp.sum(jnp.sum(acc[k], axis=1), axis=1, keepdims=True)
            sums = sums + jnp.where(lanes == 2 * (STEPS * which + s) + k, total, 0.0)

    def spread(value, gather, send, recv, me, count, where):
        gather[me] = value
        for offset in range(1, count):
            pltpu.make_async_remote_copy(
                gather.at[me], gather.at[me], send, recv, device_id=where(offset), device_id_type=MESH).start()

    def collect(gather, recv, count):
        arrived(gather.at[pl.ds(0, count - 1)], recv)
        total = gather[0]
        for k in range(1, count):
            total = total + gather[k]
        return total

    def finish(p):
        to_high(STEPS - 1, p).wait_recv()
        for i in range(tiles):
            part = pl.ds(ROWS * i, ROWS)
            last[p, nx - 1, part] = last[p, nx - 1, part] - scale * fields[STEPS - 1][p, nx + 1, part]

    sums = jnp.sum(sums, axis=0, keepdims=True)
    spread(sums, gather_x, gxs_sem, gxr_sem, me_x, count_x, at_x)

    @pl.loop(n_probes - gate, n_probes)
    def _(p):
        to_high(STEPS - 1, p).start()

    pl.loop(0, SPLIT)(finish)
    sums = collect(gather_x, gxr_sem, count_x)
    spread(sums, gather_y, gys_sem, gyr_sem, me_y, count_y, at_y)
    pl.loop(SPLIT, n_probes)(finish)
    sums = collect(gather_y, gyr_sem, count_y)
    sums = jnp.broadcast_to(sums, (n_probes, 128))
    own = sums
    for p in range(1, n_probes):
        own = jnp.where(which == p, pltpu.roll(sums, 128 - 2 * STEPS * p, 1), own)
    mean = own / jnp.float32(sites)
    start = jnp.where(lax.rem(lanes, 2) == 0, mean[:, 0:1], mean[:, 1:2])
    moments[...] = (2.0 * mean - start)[:, :2 * STEPS]

    arrived(fields[0].at[:, pl.ds(0, 2 * STEPS)], xs_sem)
    arrived(faces, ys_sem)
    arrived(gather_x.at[pl.ds(0, count_x - 1)], gxs_sem)
    arrived(gather_y.at[pl.ds(0, count_y - 1)], gys_sem)


def write_out(last, moments, last_hbm, moments_hbm, last_sem, moments_sem):
    small = pltpu.make_async_copy(moments, moments_hbm, moments_sem)
    small.start()
    for p in range(last.shape[0]):
        pltpu.make_async_copy(last.at[p], last_hbm.at[p], last_sem).start()
    small.wait()
    pltpu.make_async_copy(last, last_hbm, last_sem).wait()


def local(counts, probes, disorder, spectrum_center, half_width):
    n_probes, nx, ny, nz = probes.shape
    sites = nx * counts[0] * ny * counts[1] * nz
    f32 = jnp.float32
    dma = pltpu.SemaphoreType.DMA
    vmem = pl.BlockSpec(memory_space=pltpu.VMEM)
    smem = pl.BlockSpec(memory_space=pltpu.SMEM)
    hbm = pl.BlockSpec(memory_space=pltpu.HBM)
    held = pl.pallas_call(
        functools.partial(kernel, counts, sites),
        out_shape=(
            pltpu.VMEM(probes.shape, f32),
            jax.ShapeDtypeStruct((n_probes, 2 * STEPS), f32),
        ),
        in_specs=[hbm, hbm, smem, smem],
        out_specs=(vmem, vmem),
        scratch_shapes=[pltpu.VMEM((n_probes, nx + 2, ny, nz), f32)] * STEPS + [
            pltpu.VMEM((nx, ny, nz), f32),
            pltpu.VMEM((STEPS, 2, n_probes, nx, 1, nz), f32),
            pltpu.VMEM((STEPS, 2, n_probes, nx, 1, nz), f32),
            pltpu.VMEM((nx, ny, nz), f32),
            pltpu.VMEM((2, n_probes, ROWS, 128), f32),
            pltpu.VMEM((counts[0], 1, 128), f32),
            pltpu.VMEM((counts[1], 1, 128), f32),
            dma,
            dma,
            dma,
            pltpu.SemaphoreType.REGULAR,
            pltpu.SemaphoreType.REGULAR,
            pltpu.SemaphoreType.REGULAR((max(counts[1].bit_length() - 2, 1),)),
            dma,
            dma,
            dma((2, n_probes)),
            dma((n_probes,)),
            dma((n_probes,)),
            dma,
            dma,
            dma,
            dma,
        ],
        compiler_params=pltpu.CompilerParams(
            collective_id=0, has_side_effects=True, vmem_limit_bytes=32 * 1024 * 1024),
        name="moments",
    )(*(pltpu.with_memory_space_constraint(x, pltpu.HBM) for x in (probes, disorder)),
      spectrum_center, half_width)
    return pl.pallas_call(
        write_out,
        out_shape=(jax.ShapeDtypeStruct(probes.shape, f32), jax.ShapeDtypeStruct((n_probes, 2 * STEPS), f32)),
        in_specs=[vmem] * 2,
        out_specs=(hbm,) * 2,
        scratch_shapes=[dma, dma],
        compiler_params=pltpu.CompilerParams(vmem_limit_bytes=8 * 1024 * 1024),
        name="write_out",
    )(*(pltpu.with_memory_space_constraint(x, pltpu.VMEM) for x in held))


def solution(mesh):
    counts = (mesh.shape["gx"], mesh.shape["gy"])
    in_specs = (P(None, "gx", "gy", None), P("gx", "gy", None), P(), P())
    out_specs = (P(None, "gx", "gy", None), P())
    return jax.shard_map(functools.partial(local, counts), mesh=mesh, in_specs=in_specs,
                         out_specs=out_specs, check_vma=False)
```

```python
import functools

import jax
import jax.numpy as jnp
from jax import lax
from jax.experimental import pallas as pl
from jax.experimental.pallas import tpu as pltpu
from jax.sharding import PartitionSpec as P

STEPS = 4
MESH = pl.DeviceIdType.MESH
ROWS = 8
LEAD = (5, 4)
GATES = (5, 6, 7, 8)
SPLIT = 2


def kernel(counts, sites, probes_hbm, disorder_hbm, center, width, last, moments, *scratch):
    fields = scratch[:STEPS]
    (disorder, near, faces, coef, acc, gather_x, gather_y, load_sem, face_sem, energy_sem, up_sem, down_sem,
     round_sem, xs_sem, ys_sem, recv_sem, low_sem, high_sem, gxs_sem, gxr_sem, gys_sem, gyr_sem) = scratch[STEPS:]
    n_probes, nx, ny, nz = probes_hbm.shape
    tiles = ny // ROWS
    assert 2 * nx % ny == 0 and 2 * STEPS <= nx + 2 and 2 * STEPS * n_probes <= 128
    count_x, count_y = counts
    me_x = lax.axis_index("gx")
    me_y = lax.axis_index("gy")

    top = count_x - 1
    gate = jnp.where(me_x == 0, GATES[0], jnp.where(me_x == 1, GATES[1], jnp.where(me_x < top, GATES[2], GATES[3])))
    if count_y & (count_y - 1):
        mates = [lax.rem(me_y + k, count_y) for k in range(1, count_y)]
        rounds = 0
    else:
        widths = [1 << k for k in range(count_y.bit_length() - 1)]
        mates = [me_y + w * (1 - 2 * lax.rem(lax.div(me_y, w), 2)) for w in widths]
        rounds = len(widths) - 1

    def at_x(offset):
        return (lax.rem(me_x + offset, count_x), me_y)

    def at_y(offset):
        return (me_x, lax.rem(me_y + offset, count_y))

    def load_face(row):
        return pltpu.make_async_copy(
            probes_hbm.at[:, pl.ds(row, 1)], fields[0].at[:, pl.ds(row + 1, 1)], face_sem)

    def load(p):
        return pltpu.make_async_copy(
            probes_hbm.at[p, pl.ds(1, nx - 2)], fields[0].at[p, pl.ds(2, nx - 2)], load_sem)

    def arrived(ref, sem):
        pltpu.make_async_copy(ref, ref, sem).wait()

    def to_high(s, p):
        final_step = s + 1 == STEPS
        return pltpu.make_async_remote_copy(
            fields[s].at[p, 1], fields[s].at[p, nx + 1], xs_sem,
            high_sem.at[p] if final_step else recv_sem.at[s % 2, p], device_id=at_x(count_x - 1), device_id_type=MESH)

    def to_low(s, p):
        return pltpu.make_async_remote_copy(
            fields[s].at[p, nx], fields[s].at[p, 0], xs_sem,
            low_sem.at[p] if s + 1 == STEPS else recv_sem.at[s % 2, p], device_id=at_x(1), device_id_type=MESH)

    def y_sends(s, p):
        return (
            pltpu.make_async_remote_copy(
                faces.at[s, 0, p], near.at[s, 1, p], ys_sem, recv_sem.at[s % 2, p],
                device_id=at_y(count_y - 1), device_id_type=MESH),
            pltpu.make_async_remote_copy(
                faces.at[s, 1, p], near.at[s, 0, p], ys_sem, recv_sem.at[s % 2, p],
                device_id=at_y(1), device_id_type=MESH),
        )

    barrier = pltpu.get_barrier_semaphore()

    @pl.when(me_x < top)
    def _():
        pl.semaphore_signal(barrier, inc=1, device_id=(me_x + 1, me_y), device_id_type=MESH)

    @pl.when(me_x > 0)
    def _():
        pl.semaphore_signal(barrier, inc=1, device_id=(me_x - 1, me_y), device_id_type=MESH)

    for mate in mates:
        pl.semaphore_signal(barrier, inc=1, device_id=(me_x, mate), device_id_type=MESH)

    for row in (0, nx - 1):
        load_face(row).start()

    @pl.loop(0, n_probes)
    def _(p):
        load(p).start()

    energy = pltpu.make_async_copy(disorder_hbm, disorder, energy_sem)
    energy.start()

    arrived(fields[0].at[:, pl.ds(0, 2)], face_sem)
    pl.semaphore_wait(barrier, len(mates) + (me_x < top).astype(jnp.int32) + (me_x > 0).astype(jnp.int32))

    def greet(k):
        for mate in mates:
            pl.semaphore_signal(round_sem.at[k], inc=1, device_id=(me_x, mate), device_id_type=MESH)

    def take_faces(p):
        def row(x, carry):
            faces[0, 0, p, x] = fields[0][p, x + 1, pl.ds(0, 1)]
            faces[0, 1, p, x] = fields[0][p, x + 1, pl.ds(ny - 1, 1)]
            return carry

        lax.fori_loop(0, nx, row, 0, unroll=4)

    if rounds:
        greet(0)

    @pl.when(me_x == 1)
    def _():
        if count_x > 2:
            pl.semaphore_signal(up_sem, inc=1, device_id=(me_x + 1, me_y), device_id_type=MESH)

    @pl.when(me_x == top - 1)
    def _():
        if count_x > 2:
            pl.semaphore_signal(down_sem, inc=1, device_id=(me_x - 1, me_y), device_id_type=MESH)

    lead = [min(k, n_probes) for k in LEAD]

    @pl.when(me_x == 0)
    def _():
        for p in range(lead[0]):
            to_low(0, p).start()

    @pl.when(me_x == top)
    def _():
        for p in range(lead[1]):
            to_high(0, p).start()

    @pl.when(jnp.logical_and(me_x > 0, me_x < top))
    def _():
        @pl.loop(0, n_probes)
        def _(p):
            to_low(0, p).start()
            to_high(0, p).start()

    arrived(fields[0].at[:, pl.ds(2, nx - 2)], load_sem)
    pl.loop(0, n_probes)(take_faces)

    def other_sends(lead, adjacent, wrapped, proof):
        if count_x > 2:
            pl.semaphore_wait(proof, 1)
        for p in range(lead, n_probes):
            wrapped(0, p - lead).start()
            adjacent(0, p).start()
        for p in range(n_probes - lead, n_probes):
            wrapped(0, p).start()

    def pass_on():
        @pl.when(jnp.logical_and(me_x > 1, me_x < top))
        def _():
            pl.semaphore_wait(up_sem, 1)
            pl.semaphore_signal(up_sem, inc=1, device_id=(me_x + 1, me_y), device_id_type=MESH)

        @pl.when(jnp.logical_and(me_x > 0, me_x < top - 1))
        def _():
            pl.semaphore_wait(down_sem, 1)
            pl.semaphore_signal(down_sem, inc=1, device_id=(me_x - 1, me_y), device_id_type=MESH)

        @pl.when(me_x == 0)
        def _():
            other_sends(lead[0], to_low, to_high, down_sem)

        @pl.when(me_x == top)
        def _():
            other_sends(lead[1], to_high, to_low, up_sem)

    for k in range(rounds):
        pl.semaphore_wait(round_sem.at[k], len(mates))
        if k + 1 < rounds:
            greet(k + 1)
        if k == 0:
            pass_on()
    if not rounds:
        pass_on()

    @pl.loop(0, n_probes)
    def _(p):
        for copy in y_sends(0, p):
            copy.start()

    scale = 2.0 / jnp.full((ROWS, nz), width[0], jnp.float32)
    middle = center[0]
    energy.wait()

    @pl.loop(0, nx)
    def _(x):
        for i in range(tiles):
            part = pl.ds(ROWS * i, ROWS)
            coef[x, part] = (disorder[x, part] - middle) * scale

    sub = lax.broadcasted_iota(jnp.int32, (ROWS, nz), 0)
    first = sub == 0
    final = sub == ROWS - 1
    lanes = lax.broadcasted_iota(jnp.int32, (n_probes, 128), 1)
    which = lax.broadcasted_iota(jnp.int32, (n_probes, 128), 0)
    sums = jnp.zeros((n_probes, 128), jnp.float32)

    def fold(v):
        parts = [v[:, 128 * j:128 * (j + 1)] for j in range(nz // 128)]
        while len(parts) > 1:
            parts = [a + b for a, b in zip(parts[::2], parts[1::2])] + (
                [parts[-1]] if len(parts) % 2 else [])
        return parts[0]

    for s in range(STEPS):
        cur = fields[s]
        final_step = s + 1 == STEPS

        @pl.loop(0, n_probes)
        def _(p):
            if final_step:
                arrived(near.at[s, :, p], recv_sem.at[s % 2, p])
            else:
                arrived(cur.at[p, pl.ds(0, 2 * nx // ny + 2)], recv_sem.at[s % 2, p])

            def row(x, carry, below_x=True, above_x=True):
                square, cross = carry
                low = jnp.broadcast_to(near[s, 0, p, x], (ROWS, nz))
                high = jnp.broadcast_to(near[s, 1, p, x], (ROWS, nz))
                here = [cur[p, x + 1, pl.ds(ROWS * i, ROWS)] for i in range(tiles)]
                down = [pltpu.roll(v, 1, 0) for v in here]
                up = [pltpu.roll(v, ROWS - 1, 0) for v in here]
                for i in range(tiles):
                    part = pl.ds(ROWS * i, ROWS)
                    v = here[i]
                    below = jnp.where(first, low if i == 0 else down[i - 1], down[i])
                    above = jnp.where(final, high if i == tiles - 1 else up[i + 1], up[i])
                    beside = below + above
                    if below_x:
                        beside = beside + cur[p, x, part]
                    if above_x:
                        beside = beside + cur[p, x + 2, part]
                    beside = beside + (pltpu.roll(v, 1, 1) + pltpu.roll(v, nz - 1, 1))
                    new = coef[x, part] * v - scale * beside
                    if s == 0:
                        new = 0.5 * new
                    else:
                        new = new - fields[s - 1][p, x + 1, part]
                    if not final_step:
                        fields[s + 1][p, x + 1, part] = new
                        if i == 0:
                            faces[s + 1, 0, p, x] = new[0:1]
                        if i == tiles - 1:
                            faces[s + 1, 1, p, x] = new[ROWS - 1:ROWS]
                    else:
                        last[p, x, part] = new
                    square = square + fold(v * v)
                    cross = cross + fold(new * v)
                return square, cross

            zero = jnp.zeros((ROWS, 128), jnp.float32)
            if final_step:
                sums_p = row(0, (zero, zero), below_x=False)
                sums_p = lax.fori_loop(1, nx - 1, row, sums_p, unroll=nx - 2)
                square, cross = row(nx - 1, sums_p, above_x=False)
            else:
                square, cross = lax.fori_loop(0, nx, row, (zero, zero), unroll=nx)
            acc[0, p] = square
            acc[1, p] = cross
            if s + 1 < STEPS:
                to_low(s + 1, p).start()
                for copy in y_sends(s + 1, p):
                    copy.start()
                if s + 2 < STEPS:
                    to_high(s + 1, p).start()

        if final_step:
            @pl.loop(0, n_probes)
            def _(p):
                to_low(s, p).wait_recv()

                @pl.when(p >= gate)
                def _():
                    to_high(s, p - gate).start()

                bond = jnp.zeros((ROWS, 128), jnp.float32)
                for i in range(tiles):
                    part = pl.ds(ROWS * i, ROWS)
                    below = scale * cur[p, 0, part]
                    last[p, 0, part] = last[p, 0, part] - below
                    bond = bond + fold(below * cur[p, 1, part])
                acc[1, p] = acc[1, p] - 2.0 * bond

        for k in range(2):
            total = jnp.sum(jnp.sum(acc[k], axis=1), axis=1, keepdims=True)
            sums = sums + jnp.where(lanes == 2 * (STEPS * which + s) + k, total, 0.0)

    def spread(value, gather, send, recv, me, count, where):
        gather[me] = value
        for offset in range(1, count):
            pltpu.make_async_remote_copy(
                gather.at[me], gather.at[me], send, recv, device_id=where(offset), device_id_type=MESH).start()

    def collect(gather, recv, count):
        arrived(gather.at[pl.ds(0, count - 1)], recv)
        total = gather[0]
        for k in range(1, count):
            total = total + gather[k]
        return total

    def finish(p):
        to_high(STEPS - 1, p).wait_recv()
        for i in range(tiles):
            part = pl.ds(ROWS * i, ROWS)
            last[p, nx - 1, part] = last[p, nx - 1, part] - scale * fields[STEPS - 1][p, nx + 1, part]

    sums = jnp.sum(sums, axis=0, keepdims=True)
    spread(sums, gather_x, gxs_sem, gxr_sem, me_x, count_x, at_x)

    @pl.loop(n_probes - gate, n_probes)
    def _(p):
        to_high(STEPS - 1, p).start()

    pl.loop(0, SPLIT)(finish)
    sums = collect(gather_x, gxr_sem, count_x)
    spread(sums, gather_y, gys_sem, gyr_sem, me_y, count_y, at_y)
    pl.loop(SPLIT, n_probes)(finish)
    sums = collect(gather_y, gyr_sem, count_y)
    sums = jnp.broadcast_to(sums, (n_probes, 128))
    own = sums
    for p in range(1, n_probes):
        own = jnp.where(which == p, pltpu.roll(sums, 128 - 2 * STEPS * p, 1), own)
    mean = own / jnp.float32(sites)
    start = jnp.where(lax.rem(lanes, 2) == 0, mean[:, 0:1], mean[:, 1:2])
    moments[...] = (2.0 * mean - start)[:, :2 * STEPS]

    arrived(fields[0].at[:, pl.ds(0, 2 * STEPS)], xs_sem)
    arrived(faces, ys_sem)
    arrived(gather_x.at[pl.ds(0, count_x - 1)], gxs_sem)
    arrived(gather_y.at[pl.ds(0, count_y - 1)], gys_sem)


def write_out(last, moments, last_hbm, moments_hbm, last_sem, moments_sem):
    small = pltpu.make_async_copy(moments, moments_hbm, moments_sem)
    small.start()
    for p in range(last.shape[0]):
        pltpu.make_async_copy(last.at[p], last_hbm.at[p], last_sem).start()
    small.wait()
    pltpu.make_async_copy(last, last_hbm, last_sem).wait()


def local(counts, probes, disorder, spectrum_center, half_width):
    n_probes, nx, ny, nz = probes.shape
    sites = nx * counts[0] * ny * counts[1] * nz
    f32 = jnp.float32
    dma = pltpu.SemaphoreType.DMA
    vmem = pl.BlockSpec(memory_space=pltpu.VMEM)
    smem = pl.BlockSpec(memory_space=pltpu.SMEM)
    hbm = pl.BlockSpec(memory_space=pltpu.HBM)
    held = pl.pallas_call(
        functools.partial(kernel, counts, sites),
        out_shape=(
            pltpu.VMEM(probes.shape, f32),
            jax.ShapeDtypeStruct((n_probes, 2 * STEPS), f32),
        ),
        in_specs=[hbm, hbm, smem, smem],
        out_specs=(vmem, vmem),
        scratch_shapes=[pltpu.VMEM((n_probes, nx + 2, ny, nz), f32)] * STEPS + [
            pltpu.VMEM((nx, ny, nz), f32),
            pltpu.VMEM((STEPS, 2, n_probes, nx, 1, nz), f32),
            pltpu.VMEM((STEPS, 2, n_probes, nx, 1, nz), f32),
            pltpu.VMEM((nx, ny, nz), f32),
            pltpu.VMEM((2, n_probes, ROWS, 128), f32),
            pltpu.VMEM((counts[0], 1, 128), f32),
            pltpu.VMEM((counts[1], 1, 128), f32),
            dma,
            dma,
            dma,
            pltpu.SemaphoreType.REGULAR,
            pltpu.SemaphoreType.REGULAR,
            pltpu.SemaphoreType.REGULAR((max(counts[1].bit_length() - 2, 1),)),
            dma,
            dma,
            dma((2, n_probes)),
            dma((n_probes,)),
            dma((n_probes,)),
            dma,
            dma,
            dma,
            dma,
        ],
        compiler_params=pltpu.CompilerParams(
            collective_id=0, has_side_effects=True, vmem_limit_bytes=32 * 1024 * 1024),
        name="moments",
    )(*(pltpu.with_memory_space_constraint(x, pltpu.HBM) for x in (probes, disorder)),
      spectrum_center, half_width)
    return pl.pallas_call(
        write_out,
        out_shape=(jax.ShapeDtypeStruct(probes.shape, f32), jax.ShapeDtypeStruct((n_probes, 2 * STEPS), f32)),
        in_specs=[vmem] * 2,
        out_specs=(hbm,) * 2,
        scratch_shapes=[dma, dma],
        compiler_params=pltpu.CompilerParams(vmem_limit_bytes=8 * 1024 * 1024),
        name="write_out",
    )(*(pltpu.with_memory_space_constraint(x, pltpu.VMEM) for x in held))


def solution(mesh):
    counts = (mesh.shape["gx"], mesh.shape["gy"])
    in_specs = (P(None, "gx", "gy", None), P("gx", "gy", None), P(), P())
    out_specs = (P(None, "gx", "gy", None), P())
    return jax.shard_map(functools.partial(local, counts), mesh=mesh, in_specs=in_specs,
                         out_specs=out_specs, check_vma=False)
```
